512 devices in a mesh: win: 64 (over z, x, y_hi), strip: 8 (over y_lo, core).
Axes of the slice: x: 4, y: 8 (y_hi: 2, y_lo: 4; y = y_hi * 4 + y_lo), z: 8, core: 2. Of those that a mesh axis runs over, the one named last changes fastest.
Arguments:
- start_states: float32 [64, 3, 128, 1024], P('win', None, 'strip'), may hold values from -1.5 to 1.5
- obs_cells: int32 [64, 4, 2048], P('win', None, 'strip'), may hold values from 0 to 16383
- obs_values: float32 [64, 4, 2048], P('win', None, 'strip'), may hold values from -1.5 to 1.5
- weighting: float32 [3, 128, 128], replicated, may hold values from -0.5 to 0.5
- live_windows: int32 [64], P('win'), may hold values 0 or 1
Outputs:
- gradient: float32 [64, 3, 128, 1024], P('win', None, 'strip')
- analysis: float32 [64, 3, 128, 1024], P('win', None, 'strip')
The draws below stay inside these ranges and needn't reach their ends.
Inputs may be any that keep to these rules, and one draw needn't show every extreme that they name: `obs_cells`: each entry indexes a cell of its own row strip as (row within the strip) * 1024 + column.
All inputs are finite; a program needn't handle non-finite values. No bound on the sum of `live_windows` on one device may be relied on, other than what follows from the above.
Results may differ from the reference program's by a relative error of at most 0.0003.
Values sent between devices are 32-bit elements; how exact they have to be, the bound alone decides.
No kernel may reach another device: no remote copies, remote signals or barrier semaphores. Data moves between devices by JAX's collectives and lax.ppermute only.
A program may use at most 64 MiB of HBM per device.

```python
import jax
import jax.numpy as jnp
from jax import lax

COLS = 1024
BLOCK = 128
ROWS_DEV = 16
STEPS = 4
OBS = 256
WINDOWS = 64
NROWS = 128
N_STRIP = 8


def place_ends(entries, key, least, largest):
    dims = entries.shape
    index_at = [jax.random.randint(jax.random.fold_in(key, axis), (), 0, dims[axis]) for axis in range(len(dims))]
    entries = entries.at[tuple(index_at)].set(least)
    longest = dims.index(max(dims))
    index_at[longest] = (index_at[longest] + 1) % dims[longest]
    return entries.at[tuple(index_at)].set(largest)


def shard_levels(stream_key, dims, pieces, low, high):
    gain, own = 1.0, jax.random.fold_in(stream_key, 6)
    for dim, shards_of in pieces:
        steps = jnp.exp(jax.random.uniform(jax.random.fold_in(own, dim), (shards_of,), jnp.float32, low / len(pieces), high / len(pieces)))
        gain = gain * jnp.repeat(steps, dims[dim] // shards_of).reshape([-1 if axis == dim else 1 for axis in range(len(dims))])
    return gain


def gaussian(stream_key, dims, scale, most, split=(), kind=jnp.bfloat16):
    values = jax.random.normal(stream_key, dims, jnp.float32) * scale
    if len(split) > 0:
        values = shard_levels(stream_key, dims, split, -0.22, 0.18) * values
    return jnp.clip(values, min=-most, max=most).astype(kind)


def setup_inputs(seed: int = 0) -> dict:
    key_list = jax.random.split(jax.random.key(seed), 6)
    return {
        "start_states": gaussian(key_list[0], (WINDOWS, 3, NROWS, COLS), 0.3, 1.5, ((0, 64), (2, 8)), jnp.float32),
        "obs_cells": place_ends(jax.random.randint(key_list[1], (WINDOWS, STEPS, OBS * N_STRIP), 0, ROWS_DEV * COLS), jax.random.fold_in(key_list[1], 1), 0, (ROWS_DEV * COLS) - 1).astype(jnp.int32),
        "obs_values": gaussian(key_list[2], (WINDOWS, STEPS, OBS * N_STRIP), 0.3, 1.5, ((0, 64), (2, 8)), jnp.float32),
        "weighting": gaussian(key_list[3], (3, BLOCK, BLOCK), BLOCK ** -0.5, 0.5, (), jnp.float32),
        "live_windows": place_ends((jax.random.randint(key_list[4], (WINDOWS,), 0, 4) < 3).astype(jnp.int32), jax.random.fold_in(key_list[4], 1), 0, 1),
    }


TIME_STEP = 0.2
DIFFUSION = 0.12
CORIOLIS = 0.5
STEP_LENGTH = 0.5

def col_diff(field):
    return (jnp.roll(field[1:-1], -1, 1) - jnp.roll(field[1:-1], 1, 1)) * 0.5

def row_diff(field):
    return (field[2:] - field[:-2]) * 0.5

def laplace(field):
    inner = field[1:-1]
    return field[2:] + field[:-2] + jnp.roll(inner, -1, 1) + jnp.roll(inner, 1, 1) - 4.0 * inner

def advance(padded):
    height, east_wind, north_wind = (padded[0], padded[1], padded[2])
    depth = 1.0 + height
    flux_east = east_wind * depth
    flux_north = north_wind * depth
    height_in, east_in, north_in = (height[1:-1], east_wind[1:-1], north_wind[1:-1])
    new_height = height_in - TIME_STEP * (col_diff(flux_east) + row_diff(flux_north)) + DIFFUSION * laplace(height)
    new_east = east_in - TIME_STEP * (col_diff(height) + east_in * col_diff(east_wind) + north_in * row_diff(east_wind)) + TIME_STEP * CORIOLIS * north_in + DIFFUSION * laplace(east_wind)
    new_north = north_in - TIME_STEP * (row_diff(height) + east_in * col_diff(north_wind) + north_in * row_diff(north_wind)) - TIME_STEP * CORIOLIS * east_in + DIFFUSION * laplace(north_wind)
    return jnp.stack([new_height, new_east, new_north])

def advance_whole(state):
    return advance(jnp.pad(state, ((0, 0), (1, 1), (0, 0))))

def weigh(defect, weighting):
    fields, rows, cols = defect.shape
    width = weighting.shape[1]
    blocks = defect.reshape(fields, rows, cols // width, width)
    mixed = jnp.einsum('frbi,fij->frbj', blocks, weighting, precision=lax.Precision.HIGHEST)
    return defect + mixed.reshape(fields, rows, cols)

def forcing(adjoint, state, cells, values, alive):
    rows, cols = (state.shape[1], state.shape[2])
    flat = state[0].reshape(rows * cols)
    innovation = (flat[cells] - values) * alive
    added = jnp.zeros((rows * cols,), state.dtype).at[cells].add(innovation)
    return adjoint.at[0].add(added.reshape(rows, cols))

def reference(start_states, obs_cells, obs_values, weighting, live_windows):
    strip_of = (jnp.arange(obs_cells.shape[2]) // OBS).astype(jnp.int32)
    offsets = (strip_of * (ROWS_DEV * COLS)).astype(jnp.int32)

    def run(state):
        for moment in range(STEPS):
            state = advance_whole(state)
        return state
    ends = lax.map(run, start_states)
    previous = jnp.concatenate([jnp.zeros_like(ends[:1]), ends[:-1]], 0)
    weighted = lax.map(lambda defect: weigh(defect, weighting), start_states - previous)
    following = jnp.concatenate([weighted[1:], jnp.zeros_like(weighted[:1])], 0)
    live = live_windows.astype(start_states.dtype)

    def adjoint_window(items):
        state, cells, values, alive, successor = items
        cells = (cells + offsets[None, :]).astype(jnp.int32)
        trajectory = [state]
        for moment in range(STEPS):
            trajectory.append(advance_whole(trajectory[-1]))
        adjoint = forcing(-successor, trajectory[STEPS], cells[STEPS - 1], values[STEPS - 1], alive)
        for moment in range(STEPS - 1, -1, -1):
            unused, pullback = jax.vjp(advance_whole, trajectory[moment])
            adjoint = pullback(adjoint)[0]
            if moment > 0:
                adjoint = forcing(adjoint, trajectory[moment], cells[moment - 1], values[moment - 1], alive)
        return adjoint
    adjoints = lax.map(adjoint_window, (start_states, obs_cells, obs_values, live, following))
    gradient = weighted + adjoints
    return (gradient, start_states - STEP_LENGTH * gradient)
```

```python
import jax
import jax.numpy as jnp
from jax import lax
from jax.experimental import pallas as pl
from jax.experimental.pallas import tpu as pltpu
from jax.sharding import PartitionSpec as P

TIME_STEP = 0.2
DIFFUSION = 0.12
CORIOLIS = 0.5
STEP_LENGTH = 0.5
LANES = 128
HALF_STEP = 0.5 * TIME_STEP
CENTRE = 1.0 - 4.0 * DIFFUSION
TURN = TIME_STEP * CORIOLIS


def neighbours(load, blocks, with_rows=True):
    kept = {}

    def block(b):
        key = ("c", b % blocks)
        if key not in kept:
            kept[key] = load(b % blocks)
        return kept[key]

    def turned(b, by):
        key = ("t", b % blocks, by)
        if key not in kept:
            kept[key] = pltpu.roll(block(b), by, 1)
        return kept[key]

    def get(b):
        here = block(b)
        lane = lax.broadcasted_iota(jnp.int32, here.shape, 1)
        before = jnp.where(lane == 0, turned(b - 1, 1), turned(b, 1))
        after = jnp.where(lane == LANES - 1, turned(b + 1, LANES - 1), turned(b, LANES - 1))
        above = pltpu.roll(here, 1, 0)
        below = pltpu.roll(here, here.shape[0] - 1, 0)
        return here, before, after, above, below

    return get


def columns(b):
    return pl.ds(b * LANES, LANES)


def step_forward(source, blocks, store):
    fields = [neighbours(lambda b, f=f: source(f, b), blocks) for f in range(3)]
    for b in range(blocks):
        h, hl, hr, hu, hd = fields[0](b)
        e, el, er, eu, ed = fields[1](b)
        n, nl, nr, nu, nd = fields[2](b)
        flux = (er + er * hr) - (el + el * hl) + (nd + nd * hd) - (nu + nu * hu)
        new_h = CENTRE * h - HALF_STEP * flux + DIFFUSION * ((hl + hr) + (hu + hd))
        grad_e = (hr - hl) + e * (er - el) + n * (ed - eu)
        new_e = CENTRE * e - HALF_STEP * grad_e + TURN * n + DIFFUSION * ((el + er) + (eu + ed))
        grad_n = (hd - hu) + e * (nr - nl) + n * (nd - nu)
        new_n = CENTRE * n - HALF_STEP * grad_n - TURN * e + DIFFUSION * ((nl + nr) + (nu + nd))
        store(b, (new_h, new_e, new_n))


def step_back(state, adjoint, blocks, store):
    winds = [neighbours(lambda b, f=f: state(f, b), blocks) for f in (1, 2)]
    parts = [neighbours(lambda b, f=f: adjoint(f, b), blocks) for f in range(3)]
    for b in range(blocks):
        h = state(0, b)
        e, el, er, eu, ed = winds[0](b)
        n, nl, nr, nu, nd = winds[1](b)
        p, pl_, pr, pu, pd = parts[0](b)
        q, ql, qr, qu, qd = parts[1](b)
        r, rl, rr, ru, rd = parts[2](b)
        p_col = pr - pl_
        p_row = pd - pu
        depth = 1.0 + h
        got_h = e * p_col + n * p_row + (qr - ql) + (rd - ru)
        new_h = CENTRE * p + HALF_STEP * got_h + DIFFUSION * ((pl_ + pr) + (pu + pd))
        got_e = (
            depth * p_col
            + (er * qr - el * ql)
            + (nd * qd - nu * qu)
            - q * (er - el)
            - r * (nr - nl)
        )
        new_e = CENTRE * q + HALF_STEP * got_e - TURN * r + DIFFUSION * ((ql + qr) + (qu + qd))
        got_n = (
            depth * p_row
            + (er * rr - el * rl)
            + (nd * rd - nu * ru)
            - q * (ed - eu)
            - r * (nd - nu)
        )
        new_n = CENTRE * r + HALF_STEP * got_n + TURN * q + DIFFUSION * ((rl + rr) + (ru + rd))
        store(b, (new_h, new_e, new_n))


def halves(x):
    high = x.astype(jnp.bfloat16)
    return high, (x - high.astype(jnp.float32)).astype(jnp.bfloat16)


def weigh(defect, weights, field, blocks):
    rows = defect[0].shape[0]
    stacked = jnp.concatenate(defect, axis=0)
    high, low = halves(stacked)
    product = jnp.dot(
        jnp.concatenate([high, low], axis=0), weights[field], preferred_element_type=jnp.float32
    )
    tall = rows * blocks
    mixed = (product[:tall, :LANES] + product[:tall, LANES:]) + (
        product[tall:, :LANES] + product[tall:, LANES:]
    )
    return [defect[b] + mixed[b * rows : (b + 1) * rows] for b in range(blocks)]


def inside_mask(width):
    strip = lax.axis_index("strip")
    row = lax.broadcasted_iota(jnp.int32, (8, width), 0)
    first = strip == 0
    last = strip == lax.axis_size("strip") - 1
    outside = ((row < 4) & last) | ((row >= 4) & first)
    return jnp.where(outside, 0.0, 1.0)


def observe_kernel(rows, blocks, cells, values, live, weighting, counts, sums, weights):
    steps, seen = cells.shape[1:]
    alive = live[0].astype(jnp.float32)
    for field in range(3):
        high, low = halves(weighting[field])
        weights[field] = jnp.concatenate([high, low], axis=1)
    cols_bits = LANES.bit_length() - 1
    col_blocks = blocks.bit_length() - 1
    for j in range(steps):
        cell = cells[0, j : j + 1, :]
        place = ((cell >> cols_bits) & (blocks - 1)) * rows + (cell >> (cols_bits + col_blocks))
        lane = cell & (LANES - 1)
        value = values[0, j : j + 1, :]
        tall = lax.broadcasted_iota(jnp.int32, (rows * blocks, seen), 0)
        wide = lax.broadcasted_iota(jnp.int32, (LANES, seen), 0)
        at_place = tall == place
        left = [jnp.where(at_place, 1.0, 0.0).astype(jnp.bfloat16)]
        rest = value
        for part in range(3):
            piece = rest.astype(jnp.bfloat16).astype(jnp.float32)
            left.append(jnp.where(at_place, piece, 0.0).astype(jnp.bfloat16))
            rest = rest - piece
        right = jnp.where(wide == lane, 1.0, 0.0).astype(jnp.bfloat16)
        product = lax.dot_general(
            jnp.concatenate(left, axis=0),
            right,
            (((1,), (1,)), ((), ())),
            preferred_element_type=jnp.float32,
        )
        size = rows * blocks
        count = product[:size] * alive
        total = (product[size : 2 * size] + product[2 * size : 3 * size] + product[3 * size :]) * alive
        for b in range(blocks):
            counts[j, :, columns(b)] = count[b * rows : (b + 1) * rows]
            sums[j, :, columns(b)] = total[b * rows : (b + 1) * rows]


def forward_kernel(rows, blocks, steps, start, above, below, counts, path, end):
    width = blocks * LANES
    mask = inside_mask(LANES)
    for f in range(3):
        path[0, f, 0:rows, :] = start[0, f]
        path[0, f, rows : rows + 4, :] = below[f]
        path[0, f, rows + 4 : rows + 8, :] = above[f]

    def advance(j, _):
        def store(b, new):
            for f in range(3):
                path[j + 1, f, 0:rows, columns(b)] = new[f][:rows]
                path[j + 1, f, rows : rows + 8, columns(b)] = new[f][rows:] * mask

        step_forward(lambda f, b: path[j, f, :, columns(b)], blocks, store)
        return 0

    lax.fori_loop(0, steps - 1, advance, 0)

    def store_end(b, new):
        for f in range(3):
            end[f, :, columns(b)] = new[f][:rows]

    step_forward(lambda f, b: path[steps - 1, f, :, columns(b)], blocks, store_end)


def adjoint_kernel(
    rows, blocks, steps, path, end, next_start, counts, sums, weights, own, to_next, to_prev, work
):
    mask = inside_mask(LANES)
    is_last = lax.axis_index("win") == lax.axis_size("win") - 1
    sign = jnp.where(is_last, 0.0, -1.0)
    for f in range(3):
        defect = [
            next_start[f, :, columns(b)] - end[f, :, columns(b)] for b in range(blocks)
        ]
        weighted = weigh(defect, weights, f, blocks)
        for b in range(blocks):
            start = weighted[b] * sign
            if f == 0:
                start = start + (
                    counts[steps - 1, :, columns(b)] * end[0, :, columns(b)]
                    - sums[steps - 1, :, columns(b)]
                )
            work[0, f, 0:rows, columns(b)] = start
            work[0, f, rows : rows + 8, columns(b)] = jnp.zeros((8, LANES), jnp.float32)

    def pull(i, _):
        j = steps - 1 - i

        def store(b, new):
            for f in range(3):
                mine = new[f][:rows]
                if f == 0:
                    mine = mine + (
                        counts[j - 1, :, columns(b)] * path[j, 0, 0:rows, columns(b)]
                        - sums[j - 1, :, columns(b)]
                    )
                work[i + 1, f, 0:rows, columns(b)] = mine
                work[i + 1, f, rows : rows + 8, columns(b)] = new[f][rows:] * mask

        step_back(
            lambda f, b: path[j, f, :, columns(b)],
            lambda f, b: work[i, f, :, columns(b)],
            blocks,
            store,
        )
        return 0

    lax.fori_loop(0, steps - 1, pull, 0)

    def store_own(b, new):
        for f in range(3):
            own[f, :, columns(b)] = new[f][:rows]
            to_next[f, :, columns(b)] = new[f][rows : rows + 4]
            to_prev[f, :, columns(b)] = new[f][rows + 4 :]

    step_back(
        lambda f, b: path[0, f, :, columns(b)],
        lambda f, b: work[steps - 1, f, :, columns(b)],
        blocks,
        store_own,
    )


def final_kernel(
    rows, blocks, start, previous_end, own, from_prev, from_next, weights, gradient, analysis
):
    for f in range(3):
        defect = [
            start[0, f, :, columns(b)] - previous_end[f, :, columns(b)] for b in range(blocks)
        ]
        weighted = weigh(defect, weights, f, blocks)
        for b in range(blocks):
            spill = jnp.concatenate(
                [
                    from_prev[f, :, columns(b)],
                    jnp.zeros((rows - 8, LANES), jnp.float32),
                    from_next[f, :, columns(b)],
                ],
                axis=0,
            )
            total = weighted[b] + own[f, :, columns(b)] + spill
            gradient[0, f, :, columns(b)] = total
            analysis[0, f, :, columns(b)] = start[0, f, :, columns(b)] - STEP_LENGTH * total


def call(body, outs, flops, in_specs=None, scratch=(), name=None):
    extra = {} if in_specs is None else {"in_specs": in_specs}
    return pl.pallas_call(
        body,
        out_shape=outs,
        scratch_shapes=list(scratch),
        compiler_params=pltpu.CompilerParams(vmem_limit_bytes=12 * 1024 * 1024),
        cost_estimate=pl.CostEstimate(flops=flops, bytes_accessed=1000000, transcendentals=0),
        name=name,
        **extra,
    )


def per_device(start_states, obs_cells, obs_values, weighting, live_windows):
    fields, rows, cols = start_states.shape[1:]
    steps = obs_cells.shape[1]
    blocks = cols // LANES
    frame = rows + 8
    f32 = jnp.float32
    shape = jax.ShapeDtypeStruct
    strips, windows = lax.axis_size("strip"), lax.axis_size("win")
    up = [(i, i + 1) for i in range(strips - 1)]
    down = [(j, i) for i, j in up]
    state = start_states[0]

    next_start = lax.ppermute(state, "win", [(i + 1, i) for i in range(windows - 1)])
    above = lax.ppermute(state[:, rows - 4 :], "strip", up)
    below = lax.ppermute(state[:, :4], "strip", down)

    whole = pl.BlockSpec(memory_space=pltpu.VMEM)
    counts, sums, weights = call(
        lambda *refs: observe_kernel(rows, blocks, *refs),
        (
            shape((steps, rows, cols), f32),
            shape((steps, rows, cols), f32),
            shape((fields, LANES, 2 * LANES), jnp.bfloat16),
        ),
        4 * 10**9,
        in_specs=[whole, whole, pl.BlockSpec(memory_space=pltpu.SMEM), whole],
        name="observe",
    )(obs_cells, obs_values, live_windows, weighting)
    path, end = call(
        lambda *refs: forward_kernel(rows, blocks, steps, *refs),
        (shape((steps, fields, frame, cols), f32), shape((fields, rows, cols), f32)),
        2 * 10**9,
        name="forward",
    )(start_states, above, below, counts)
    previous_end = lax.ppermute(end, "win", [(i, i + 1) for i in range(windows - 1)])
    own, to_next, to_prev = call(
        lambda *refs: adjoint_kernel(rows, blocks, steps, *refs),
        (
            shape((fields, rows, cols), f32),
            shape((fields, 4, cols), f32),
            shape((fields, 4, cols), f32),
        ),
        4 * 10**9,
        scratch=[pltpu.VMEM((steps, fields, frame, cols), f32)],
        name="adjoint",
    )(path, end, next_start, counts, sums, weights)
    from_prev = lax.ppermute(to_next, "strip", up)
    from_next = lax.ppermute(to_prev, "strip", down)
    gradient, analysis = call(
        lambda *refs: final_kernel(rows, blocks, *refs),
        (shape(start_states.shape, f32), shape(start_states.shape, f32)),
        10**9,
        name="final",
    )(start_states, previous_end, own, from_prev, from_next, weights)
    return gradient, analysis


def solution(mesh):
    placed = (
        P("win", None, "strip", None),
        P("win", None, "strip"),
        P("win", None, "strip"),
        P(),
        P("win"),
    )
    return jax.shard_map(
        per_device,
        mesh=mesh,
        in_specs=placed,
        out_specs=(P("win", None, "strip", None), P("win", None, "strip", None)),
        check_vma=False,
    )
```
